256 devices in a mesh: pq: 8 (over z_hi, x), rs: 32 (over y, z_lo, core).
Axes of the slice: x: 4, y: 4, z: 8 (z_hi: 2, z_lo: 4; z = z_hi * 4 + z_lo), core: 2. Of those that a mesh axis runs over, the one named last changes fastest.
Arguments:
- integrals: bfloat16 [512, 1152, 1152], P('pq', 'rs'), may hold values from -6 to 6
- coeff: bfloat16 [1152, 896], P('rs', 'pq'), may hold values from -0.1875 to 0.1875
Outputs:
- half_mo: bfloat16 [512, 896, 896], P('pq', 'rs')
The draws below stay inside these ranges and needn't reach their ends.
All inputs are finite; a program needn't handle non-finite values.
Results may differ from the reference program's by a relative error of at most 0.0049.
Values may be sent and summed in bfloat16 or wider, within the bound.
A program may use at most 128 MiB of HBM per device.

```python
import jax
import jax.numpy as jnp
from jax import lax

NBASIS = 1152
NORB = 896
PAIRS = 512


def block_scale(own_key, dims, split, smallest, top_value):
    factor_of, own = 1.0, jax.random.fold_in(own_key, 6)
    for dim, parts in split:
        steps = jnp.exp(jax.random.uniform(jax.random.fold_in(own, dim), (parts,), jnp.float32, smallest / len(split), top_value / len(split)))
        factor_of = factor_of * jnp.repeat(steps, dims[dim] // parts).reshape([-1 if axis == dim else 1 for axis in range(len(dims))])
    return factor_of


def noise(own_key, shape, width, bound, cuts=(), kind=jnp.bfloat16):
    drawn = width * jax.random.normal(own_key, shape, jnp.float32)
    if cuts:
        drawn = drawn * block_scale(own_key, shape, cuts, -0.22, 0.18)
    return jnp.clip(drawn, -bound, bound).astype(kind)


def setup_inputs(seed: int = 0) -> dict:
    splits = jax.random.split(jax.random.key(seed), 3)
    return {
        "integrals": noise(splits[0], (PAIRS, NBASIS, NBASIS), 1.0, 6.0, ((0, 8), (1, 32))),
        "coeff": noise(splits[1], (NBASIS, NORB), NBASIS ** -0.5, 0.1875, ((0, 32), (1, 8))),
    }


def reference(integrals, coeff):
    pairs = integrals.shape[0]
    flat = integrals.reshape(pairs * NBASIS, NBASIS)
    first = jnp.dot(flat, coeff, preferred_element_type=jnp.float32).astype(jnp.bfloat16)
    first = first.reshape(pairs, NBASIS, NORB)

    def one_row(block):
        return jnp.dot(block.T, coeff, preferred_element_type=jnp.float32).astype(jnp.bfloat16)

    return lax.map(one_row, first)
```

```python
import functools
import jax
import jax.numpy as jnp
from jax import lax
from jax.experimental import pallas as pl
from jax.experimental.pallas import tpu as pltpu
from jax.sharding import PartitionSpec as P

MESH = pl.DeviceIdType.MESH
BF16 = jnp.bfloat16
F32 = jnp.float32


def swapped(tile):
    rows = lax.broadcasted_iota(jnp.int32, tile.shape, 0) % 2
    lanes = lax.broadcasted_iota(jnp.int32, tile.shape, 1) // 64
    turned = pltpu.roll(tile, 64, 1)
    above = pltpu.roll(turned, tile.shape[0] - 1, 0)
    below = pltpu.roll(turned, 1, 0)
    return jnp.where(rows == lanes, tile, jnp.where(rows == 0, above, below))


def kernel(i_hbm, pt_hbm, c_hbm, o_hbm, i_v, pt_v, c_v, s_v, r_v, o_v, in_sems, out_sems, send_sems, recv_sems):
    me = lax.axis_index("rs")
    loads = [
        pltpu.make_async_copy(src, dst, in_sems.at[n])
        for n, (src, dst) in enumerate(((i_hbm, i_v), (pt_hbm, pt_v), (c_hbm, c_v)))
    ]
    for load in loads:
        load.start()
    barrier = pltpu.get_barrier_semaphore()

    def greet(k, _):
        pl.semaphore_signal(barrier, inc=1, device_id={"rs": lax.rem(me + k, 32)}, device_id_type=MESH)
        return 0

    lax.fori_loop(1, 32, greet, 0)
    loads[0].wait()
    loads[1].wait()
    pl.semaphore_wait(barrier, 31)

    def send(q, d):
        return pltpu.make_async_remote_copy(
            src_ref=s_v.at[q, d],
            dst_ref=r_v.at[q, :, me],
            send_sem=send_sems.at[q],
            recv_sem=recv_sems.at[q],
            device_id={"rs": d},
            device_id_type=MESH,
        )

    def first(q, _):
        def columns(g, _):
            acc = lax.dot_general(
                pt_v[q], i_v[pl.ds(pl.multiple_of(g * 256, 256), 256), :], (((1,), (1,)), ((), ())), preferred_element_type=F32
            )
            for h in range(2):
                tile = swapped(acc[:, h * 128 : (h + 1) * 128]).astype(BF16)
                s_v[q, :, :, 2 * g + h] = tile.reshape(32, 2, 2, 128)
            return 0

        lax.fori_loop(0, 9, columns, 0)

        def issue(k, _):
            send(q, lax.rem(me + k, 32)).start()
            return 0

        lax.fori_loop(1, 32, issue, 0)
        r_v[q, :, me] = s_v[q, me]
        return 0

    lax.fori_loop(0, 7, first, 0)
    loads[2].wait()

    def second(q, _):
        pltpu.make_async_copy(r_v.at[q, :, pl.ds(0, 31)], r_v.at[q, :, pl.ds(0, 31)], recv_sems.at[q]).wait()
        for lp in range(2):
            x = r_v[q, lp].reshape(1152, 128)
            acc = lax.dot_general(x, c_v[...], (((0,), (0,)), ((), ())), preferred_element_type=F32)
            o_v[q, pl.ds(lp * 128, 128), :] = acc.astype(BF16)
        pltpu.make_async_copy(o_v.at[q], o_hbm.at[q], out_sems.at[q]).start()
        return 0

    lax.fori_loop(0, 7, second, 0)

    def drain(q, _):
        pltpu.make_async_copy(o_v.at[q], o_hbm.at[q], out_sems.at[q]).wait()
        pltpu.make_async_copy(s_v.at[q, pl.ds(0, 31)], s_v.at[q, pl.ds(0, 31)], send_sems.at[q]).wait()
        return 0

    lax.fori_loop(0, 7, drain, 0)


def transform(i2d, pt, c):
    any_ = pl.BlockSpec(memory_space=pl.ANY)
    return pl.pallas_call(
        kernel,
        out_shape=jax.ShapeDtypeStruct((7, 256, 896), BF16),
        in_specs=[any_] * 3,
        out_specs=any_,
        scratch_shapes=[
            pltpu.VMEM((2304, 1152), BF16),
            pltpu.VMEM((7, 128, 1152), BF16),
            pltpu.VMEM((1152, 896), BF16),
            pltpu.VMEM((7, 32, 2, 18, 2, 128), BF16),
            pltpu.VMEM((7, 2, 32, 18, 2, 128), BF16),
            pltpu.VMEM((7, 256, 896), BF16),
            pltpu.SemaphoreType.DMA((3,)),
            pltpu.SemaphoreType.DMA((7,)),
            pltpu.SemaphoreType.DMA((7,)),
            pltpu.SemaphoreType.DMA((7,)),
        ],
        compiler_params=pltpu.CompilerParams(collective_id=0, has_side_effects=True, vmem_limit_bytes=60 * 2**20),
        name="half",
    )(i2d, pt, c)


def on_device(integrals, coeff):
    i2d = integrals.transpose(1, 0, 2).reshape(2304, 1152)
    strip = lax.all_gather(coeff, "pq", axis=1, tiled=True)
    panel = lax.all_gather(strip, "rs", axis=0, tiled=True)
    pt = panel.T.reshape(32, 7, 4, 1152).transpose(1, 0, 2, 3).reshape(7, 128, 1152)
    out = transform(i2d, pt, panel)
    return out.reshape(28, 64, 896).transpose(1, 0, 2)


def solution(mesh):
    placed = (P("pq", "rs", None), P("rs", "pq"))
    return jax.shard_map(on_device, mesh=mesh, in_specs=placed, out_specs=P("pq", "rs", None), check_vma=False)
```

```python
import jax
import jax.numpy as jnp
from jax import lax
from jax.experimental import pallas as pl
from jax.experimental.pallas import tpu as pltpu
from jax.sharding import PartitionSpec as P

MESH = pl.DeviceIdType.MESH
BF16 = jnp.bfloat16
F32 = jnp.float32
CHUNKS = 7


def one_hot(shape, column_of_row):
    rows = lax.broadcasted_iota(jnp.int32, shape, 0)
    columns = lax.broadcasted_iota(jnp.int32, shape, 1)
    return jnp.where(column_of_row(rows) == columns, 1.0, 0.0).astype(BF16)


def swapped(tile):
    rows = lax.broadcasted_iota(jnp.int32, tile.shape, 0) % 2
    lanes = lax.broadcasted_iota(jnp.int32, tile.shape, 1) // 64
    turned = pltpu.roll(tile, 64, 1)
    above = pltpu.roll(turned, tile.shape[0] - 1, 0)
    below = pltpu.roll(turned, 1, 0)
    return jnp.where(rows == lanes, tile, jnp.where(rows == 0, above, below))


def kernel(
    i_hbm, b_hbm, o_hbm,
    i_v, blk_v, b_v, z_v, at_v, g_v, pt_v, perm_v, c_v, s_v, r_v, o_v,
    in_sems, out_sems, zsend, zrecv, gsend, grecv, send_sems, recv_sems,
):
    pq, rs = lax.axis_index("pq"), lax.axis_index("rs")
    zh, x = pq // 4, pq % 4
    y, zl, core = rs // 8, (rs // 2) % 4, rs % 2
    z = zh * 4 + zl

    def column_peer(k):
        pz, pc = (z + k // 2) % 8, (core + k) % 2
        return {"pq": (pz // 4) * 4 + x, "rs": y * 8 + (pz % 4) * 2 + pc}

    def plane_peer(k):
        py, px = (y + k // 4) % 4, (x + k) % 4
        return {"pq": zh * 4 + px, "rs": py * 8 + zl * 2 + core}

    def row_peer(k):
        return {"rs": (rs + k) % 32}

    load_i = pltpu.make_async_copy(i_hbm, i_v, in_sems.at[0])
    load_b = pltpu.make_async_copy(b_hbm, blk_v, in_sems.at[1])
    load_b.start()
    load_i.start()
    barrier = pltpu.get_barrier_semaphore()

    def greet(peer):
        def one(k, _):
            pl.semaphore_signal(barrier, inc=1, device_id=peer(k), device_id_type=MESH)
            return 0

        return one

    z_v[...] = jnp.zeros(z_v.shape, BF16)
    b_v[...] = jnp.zeros(b_v.shape, BF16)
    lax.fori_loop(1, 16, greet(column_peer), 0)
    lax.fori_loop(1, 16, greet(plane_peer), 0)
    lax.fori_loop(1, 32, greet(row_peer), 0)

    load_b.wait()
    b_v[:, :, 0:112] = blk_v[...].reshape(9, 4, 112)
    spot = zh * 96 + y * 8 + (zl * 2 + core) * 9
    z_v[pl.ds(spot, 9)] = b_v[...]
    pl.semaphore_wait(barrier, 61)

    def send_block(k, _):
        pltpu.make_async_remote_copy(
            src_ref=b_v, dst_ref=z_v.at[pl.ds(spot, 9)], send_sem=zsend, recv_sem=zrecv,
            device_id=column_peer(k), device_id_type=MESH,
        ).start()
        return 0

    lax.fori_loop(1, 16, send_block, 0)
    order = one_hot((128, 128), lambda n: jnp.where(n < 112, ((n // 4) % 4) * 28 + (n // 16) * 4 + n % 4, -1))
    perm_v[...] = one_hot(
        perm_v.shape, lambda n: ((n // 16) % 8) * 112 + ((n // 4) % 4) * 28 + (n // 128) * 4 + n % 4
    )
    pltpu.make_async_copy(z_v.at[pl.ds(0, 135)], z_v.at[pl.ds(0, 135)], zrecv).wait()
    mine = y * 4 + x
    for h in range(2):
        strip = z_v[pl.ds(h * 96, 96)].reshape(384, 128)
        turned = lax.dot_general(order, strip, (((1,), (1,)), ((), ())), preferred_element_type=F32).astype(BF16)
        for q in range(CHUNKS):
            at_v[q, h] = turned[q * 16 : (q + 1) * 16]
            g_v[q, mine, h] = turned[q * 16 : (q + 1) * 16]

    def spread(q):
        def one(k, _):
            pltpu.make_async_remote_copy(
                src_ref=at_v.at[q], dst_ref=g_v.at[q, mine], send_sem=gsend.at[q], recv_sem=grecv.at[q],
                device_id=plane_peer(k), device_id_type=MESH,
            ).start()
            return 0

        lax.fori_loop(1, 16, one, 0)

    spread(0)
    spread(1)
    load_i.wait()

    def first(q, _):
        pltpu.make_async_copy(g_v.at[q, pl.ds(0, 15)], g_v.at[q, pl.ds(0, 15)], grecv.at[q]).wait()
        rows = pl.ds(pl.multiple_of(q * 128, 128), 128)
        windows = [
            jnp.concatenate([g_v[q, w * 4 + px, h] for h in range(2) for px in range(4)], axis=0) for w in range(4)
        ]
        for t in range(9):
            parts = [windows[w][:, (t - 2 * w) * 128 : (t - 2 * w + 1) * 128] for w in range(4) if 0 <= t - 2 * w < 3]
            pt_v[rows, t * 128 : (t + 1) * 128] = sum(parts[1:], parts[0])

        def columns(g, _):
            acc = lax.dot_general(
                pt_v[rows, :], i_v[pl.ds(pl.multiple_of(g * 256, 256), 256), :], (((1,), (1,)), ((), ())),
                preferred_element_type=F32,
            )
            for h in range(2):
                tile = swapped(acc[:, h * 128 : (h + 1) * 128]).astype(BF16)
                s_v[q, :, :, 2 * g + h] = tile.reshape(32, 2, 2, 128)
            return 0

        lax.fori_loop(0, 9, columns, 0)

        def issue(k, _):
            d = (rs + k) % 32
            pltpu.make_async_remote_copy(
                src_ref=s_v.at[q, d], dst_ref=r_v.at[q, :, rs], send_sem=send_sems.at[q], recv_sem=recv_sems.at[q],
                device_id={"rs": d}, device_id_type=MESH,
            ).start()
            return 0

        lax.fori_loop(1, 32, issue, 0)
        r_v[q, :, rs] = s_v[q, rs]

        @pl.when(q < CHUNKS - 2)
        def _():
            spread(q + 2)

        return 0

    lax.fori_loop(0, CHUNKS, first, 0)

    def natural(g, _):
        rows = pl.ds(pl.multiple_of(g * 128, 128), 128)
        acc = lax.dot_general(pt_v[:, rows], perm_v[...], (((0,), (0,)), ((), ())), preferred_element_type=F32)
        c_v[rows, :] = acc.astype(BF16)
        return 0

    lax.fori_loop(0, 9, natural, 0)

    def second(q, _):
        pltpu.make_async_copy(r_v.at[q, :, pl.ds(0, 31)], r_v.at[q, :, pl.ds(0, 31)], recv_sems.at[q]).wait()
        for lp in range(2):
            tiles = r_v[q, lp].reshape(NBASIS, 128)
            acc = lax.dot_general(tiles, c_v[...], (((0,), (0,)), ((), ())), preferred_element_type=F32)
            o_v[q, pl.ds(lp * 128, 128), :] = acc.astype(BF16)
        pltpu.make_async_copy(o_v.at[q], o_hbm.at[q], out_sems.at[q]).start()
        return 0

    lax.fori_loop(0, CHUNKS, second, 0)

    def drain(q, _):
        pltpu.make_async_copy(o_v.at[q], o_hbm.at[q], out_sems.at[q]).wait()
        pltpu.make_async_copy(s_v.at[q, pl.ds(0, 31)], s_v.at[q, pl.ds(0, 31)], send_sems.at[q]).wait()
        pltpu.make_async_copy(g_v.at[q, pl.ds(0, 15)], g_v.at[q, pl.ds(0, 15)], gsend.at[q]).wait()
        return 0

    lax.fori_loop(0, CHUNKS, drain, 0)
    pltpu.make_async_copy(z_v.at[pl.ds(0, 135)], z_v.at[pl.ds(0, 135)], zsend).wait()


NBASIS = 1152
NORB = 896


def transform(flat, block):
    anywhere = pl.BlockSpec(memory_space=pl.ANY)
    dma = pltpu.SemaphoreType.DMA
    return pl.pallas_call(
        kernel,
        out_shape=jax.ShapeDtypeStruct((CHUNKS, 256, NORB), BF16),
        in_specs=[anywhere] * 2,
        out_specs=anywhere,
        scratch_shapes=[
            pltpu.VMEM((2304, NBASIS), BF16),
            pltpu.VMEM((36, 112), BF16),
            pltpu.VMEM((9, 4, 128), BF16),
            pltpu.VMEM((192, 4, 128), BF16),
            pltpu.VMEM((CHUNKS, 2, 16, 384), BF16),
            pltpu.VMEM((CHUNKS, 16, 2, 16, 384), BF16),
            pltpu.VMEM((NORB, NBASIS), BF16),
            pltpu.VMEM((NORB, NORB), BF16),
            pltpu.VMEM((NBASIS, NORB), BF16),
            pltpu.VMEM((CHUNKS, 32, 2, 18, 2, 128), BF16),
            pltpu.VMEM((CHUNKS, 2, 32, 18, 2, 128), BF16),
            pltpu.VMEM((CHUNKS, 256, NORB), BF16),
            dma((2,)),
            dma((CHUNKS,)),
            dma,
            dma,
            dma((CHUNKS,)),
            dma((CHUNKS,)),
            dma((CHUNKS,)),
            dma((CHUNKS,)),
        ],
        compiler_params=pltpu.CompilerParams(collective_id=0, has_side_effects=True, vmem_limit_bytes=60 * 2**20),
        name="half",
    )(flat, block)


def on_device(integrals, coeff):
    flat = integrals.transpose(1, 0, 2).reshape(2304, NBASIS)
    return transform(flat, coeff).reshape(28, 64, NORB).transpose(1, 0, 2)


def solution(mesh):
    placed = (P("pq", "rs", None), P("rs", "pq"))
    return jax.shard_map(on_device, mesh=mesh, in_specs=placed, out_specs=P("pq", "rs", None), check_vma=False)
```

```python
import jax
import jax.numpy as jnp
from jax import lax
from jax.experimental import pallas as pl
from jax.experimental.pallas import tpu as pltpu
from jax.sharding import PartitionSpec as P

MESH = pl.DeviceIdType.MESH
BF16 = jnp.bfloat16
F32 = jnp.float32
CHUNKS = 14
AHEAD = 4


def one_hot(shape, column_of_row):
    rows = lax.broadcasted_iota(jnp.int32, shape, 0)
    columns = lax.broadcasted_iota(jnp.int32, shape, 1)
    return jnp.where(column_of_row(rows) == columns, 1.0, 0.0).astype(BF16)


def swapped(tile):
    rows = lax.broadcasted_iota(jnp.int32, tile.shape, 0) % 2
    lanes = lax.broadcasted_iota(jnp.int32, tile.shape, 1) // 64
    turned = pltpu.roll(tile, 64, 1)
    above = pltpu.roll(turned, tile.shape[0] - 1, 0)
    below = pltpu.roll(turned, 1, 0)
    return jnp.where(rows == lanes, tile, jnp.where(rows == 0, above, below))


def kernel(
    i_hbm, b_ref, o_ref,
    i_v, b_v, z_v, at_v, g_v, pt_v, perm_v, c_v, s_v, r_v,
    in_sems, zsend, zrecv, gsend, grecv, send_sems, recv_sems,
):
    pq, rs = lax.axis_index("pq"), lax.axis_index("rs")
    zh, x = pq // 4, pq % 4
    y, zl, core = rs // 8, (rs // 2) % 4, rs % 2
    z = zh * 4 + zl

    def column_peer(k):
        pz, pc = (z + k // 2) % 8, (core + k) % 2
        return {"pq": (pz // 4) * 4 + x, "rs": y * 8 + (pz % 4) * 2 + pc}

    def plane_peer(k):
        py, px = (y + k // 4) % 4, (x + k) % 4
        return {"pq": zh * 4 + px, "rs": py * 8 + zl * 2 + core}

    def row_peer(k):
        return {"rs": (rs + k) % 32}

    load_i = pltpu.make_async_copy(i_hbm, i_v, in_sems.at[0])
    load_i.start()
    barrier = pltpu.get_barrier_semaphore()

    def greet(peer):
        def one(k, _):
            pl.semaphore_signal(barrier, inc=1, device_id=peer(k), device_id_type=MESH)
            return 0

        return one

    z_v[...] = jnp.zeros(z_v.shape, BF16)
    b_v[...] = jnp.zeros(b_v.shape, BF16)
    lax.fori_loop(1, 16, greet(column_peer), 0)
    lax.fori_loop(1, 16, greet(plane_peer), 0)
    lax.fori_loop(1, 32, greet(row_peer), 0)

    b_v[:, :, 0:112] = b_ref[...].reshape(9, 4, 112)
    spot = zh * 96 + y * 8 + (zl * 2 + core) * 9
    z_v[pl.ds(spot, 9)] = b_v[...]
    pl.semaphore_wait(barrier, 61)

    def send_block(k, _):
        pltpu.make_async_remote_copy(
            src_ref=b_v, dst_ref=z_v.at[pl.ds(spot, 9)], send_sem=zsend, recv_sem=zrecv,
            device_id=column_peer(k), device_id_type=MESH,
        ).start()
        return 0

    lax.fori_loop(1, 16, send_block, 0)
    order = one_hot((128, 128), lambda n: jnp.where(n < 112, ((n // 2) % 4) * 28 + (n // 8) * 2 + n % 2, -1))
    perm_v[...] = one_hot(
        perm_v.shape, lambda n: ((n // 8) % 8) * 112 + ((n // 2) % 4) * 28 + (n // 64) * 2 + n % 2
    )
    pltpu.make_async_copy(z_v.at[pl.ds(0, 135)], z_v.at[pl.ds(0, 135)], zrecv).wait()
    mine = y * 4 + x

    def spread(q):
        def one(k, _):
            pltpu.make_async_remote_copy(
                src_ref=at_v.at[q], dst_ref=g_v.at[q, mine], send_sem=gsend.at[q], recv_sem=grecv.at[q],
                device_id=plane_peer(k), device_id_type=MESH,
            ).start()
            return 0

        lax.fori_loop(1, 16, one, 0)

    turned = [
        lax.dot_general(
            order, z_v[pl.ds(h * 96, 96)].reshape(384, 128), (((1,), (1,)), ((), ())), preferred_element_type=F32
        ).astype(BF16)
        for h in range(2)
    ]

    def keep(q):
        for h in range(2):
            at_v[q, h] = turned[h][q * 8 : (q + 1) * 8]

    keep(0)
    spread(0)
    for q in range(1, CHUNKS):
        keep(q)
    for q in range(1, AHEAD):
        spread(q)
    g_v[:, mine] = at_v[...]
    load_i.wait()

    def first(q, _):
        pltpu.make_async_copy(g_v.at[q, pl.ds(0, 15)], g_v.at[q, pl.ds(0, 15)], grecv.at[q]).wait()
        rows = pl.ds(pl.multiple_of(q * 64, 64), 64)
        windows = [
            jnp.concatenate([g_v[q, w * 4 + px, h] for h in range(2) for px in range(4)], axis=0) for w in range(4)
        ]
        for t in range(9):
            parts = [windows[w][:, (t - 2 * w) * 128 : (t - 2 * w + 1) * 128] for w in range(4) if 0 <= t - 2 * w < 3]
            pt_v[rows, t * 128 : (t + 1) * 128] = sum(parts[1:], parts[0])

        def columns(u, _):
            for v in range(3):
                g = u * 3 + v
                acc = lax.dot_general(
                    pt_v[rows, :], i_v[pl.ds(pl.multiple_of(g * 256, 256), 256), :], (((1,), (1,)), ((), ())),
                    preferred_element_type=F32,
                )
                for h in range(2):
                    tile = swapped(acc[:, h * 128 : (h + 1) * 128]).astype(BF16)
                    s_v[q, :, 2 * g + h] = tile.reshape(32, 2, 128)
            return 0

        lax.fori_loop(0, 3, columns, 0)

        def issue(k, _):
            d = (rs + k) % 32
            pltpu.make_async_remote_copy(
                src_ref=s_v.at[q, d], dst_ref=r_v.at[q, rs], send_sem=send_sems.at[q], recv_sem=recv_sems.at[q],
                device_id={"rs": d}, device_id_type=MESH,
            ).start()
            return 0

        lax.fori_loop(1, 32, issue, 0)
        r_v[q, rs] = s_v[q, rs]

        @pl.when(q < CHUNKS - AHEAD)
        def _():
            spread(q + AHEAD)

        return 0

    lax.fori_loop(0, CHUNKS, first, 0)

    def natural(g, _):
        rows = pl.ds(pl.multiple_of(g * 128, 128), 128)
        acc = lax.dot_general(pt_v[:, rows], perm_v[...], (((0,), (0,)), ((), ())), preferred_element_type=F32)
        c_v[rows, :] = acc.astype(BF16)
        return 0

    lax.fori_loop(0, 9, natural, 0)

    def second(q, _):
        pltpu.make_async_copy(r_v.at[q, pl.ds(0, 31)], r_v.at[q, pl.ds(0, 31)], recv_sems.at[q]).wait()
        tiles = r_v[q].reshape(NBASIS, 128)
        acc = lax.dot_general(tiles, c_v[...], (((0,), (0,)), ((), ())), preferred_element_type=F32)
        o_ref[q] = acc.astype(BF16)
        return 0

    lax.fori_loop(0, CHUNKS, second, 0)

    def drain(q, _):
        pltpu.make_async_copy(s_v.at[q, pl.ds(0, 31)], s_v.at[q, pl.ds(0, 31)], send_sems.at[q]).wait()
        pltpu.make_async_copy(g_v.at[q, pl.ds(0, 15)], g_v.at[q, pl.ds(0, 15)], gsend.at[q]).wait()
        return 0

    lax.fori_loop(0, CHUNKS, drain, 0)
    pltpu.make_async_copy(z_v.at[pl.ds(0, 135)], z_v.at[pl.ds(0, 135)], zsend).wait()


NBASIS = 1152
NORB = 896


def transform(flat, block):
    far = pl.BlockSpec(memory_space=pltpu.HBM)
    dma = pltpu.SemaphoreType.DMA
    return pl.pallas_call(
        kernel,
        out_shape=jax.ShapeDtypeStruct((CHUNKS, 128, NORB), BF16),
        in_specs=[far, pl.BlockSpec(memory_space=pltpu.VMEM)],
        out_specs=pl.BlockSpec(memory_space=pltpu.VMEM),
        scratch_shapes=[
            pltpu.VMEM((2304, NBASIS), BF16),
            pltpu.VMEM((9, 4, 128), BF16),
            pltpu.VMEM((192, 4, 128), BF16),
            pltpu.VMEM((CHUNKS, 2, 8, 384), BF16),
            pltpu.VMEM((CHUNKS, 16, 2, 8, 384), BF16),
            pltpu.VMEM((NORB, NBASIS), BF16),
            pltpu.VMEM((NORB, NORB), BF16),
            pltpu.VMEM((NBASIS, NORB), BF16),
            pltpu.VMEM((CHUNKS, 32, 18, 2, 128), BF16),
            pltpu.VMEM((CHUNKS, 32, 18, 2, 128), BF16),
            dma((1,)),
            dma,
            dma,
            dma((CHUNKS,)),
            dma((CHUNKS,)),
            dma((CHUNKS,)),
            dma((CHUNKS,)),
        ],
        compiler_params=pltpu.CompilerParams(collective_id=0, has_side_effects=True, vmem_limit_bytes=48 * 2**20),
        name="half",
    )(flat, block)


def on_device(integrals, coeff):
    flat = integrals.transpose(1, 0, 2).reshape(2304, NBASIS)
    return transform(flat, coeff).reshape(28, 64, NORB).transpose(1, 0, 2)


def solution(mesh):
    placed = (P("pq", "rs", None), P("rs", "pq"))
    return jax.shard_map(on_device, mesh=mesh, in_specs=placed, out_specs=P("pq", "rs", None), check_vma=False)
```

```python
import functools

import jax
import jax.numpy as jnp
from jax import lax
from jax.experimental import pallas as pl
from jax.experimental.pallas import tpu as pltpu
from jax.sharding import PartitionSpec as P

MESH = pl.DeviceIdType.MESH
BF16 = jnp.bfloat16
F32 = jnp.float32
CHUNKS = 14
DIRECT = 3


def one_hot(shape, column_of_row):
    rows = lax.broadcasted_iota(jnp.int32, shape, 0)
    columns = lax.broadcasted_iota(jnp.int32, shape, 1)
    return jnp.where(column_of_row(rows) == columns, 1.0, 0.0).astype(BF16)


def swapped(tile):
    rows = lax.broadcasted_iota(jnp.int32, tile.shape, 0) % 2
    lanes = lax.broadcasted_iota(jnp.int32, tile.shape, 1) // 64
    turned = pltpu.roll(tile, 64, 1)
    above = pltpu.roll(turned, tile.shape[0] - 1, 0)
    below = pltpu.roll(turned, 1, 0)
    return jnp.where(rows == lanes, tile, jnp.where(rows == 0, above, below))


def kernel(
    i_hbm, b_hbm, o_ref,
    i_v, blk_v, b_v, z_v, at_v, g_v, pt_v, perm_v, c_v, s_v, r_v,
    in_sems, zsend, zrecv, ysend, yrecv, gsend, grecv, send_sems, recv_sems,
):
    pq, rs = lax.axis_index("pq"), lax.axis_index("rs")
    zh, x = pq // 4, pq % 4
    y, zl, core = rs // 8, (rs // 2) % 4, rs % 2
    z = zh * 4 + zl

    def column_peer(k):
        pz, pc = (z + k // 2) % 8, (core + k) % 2
        return {"pq": (pz // 4) * 4 + x, "rs": y * 8 + (pz % 4) * 2 + pc}

    def plane_peer(k):
        py, px = (y + k // 4) % 4, (x + k) % 4
        return {"pq": zh * 4 + px, "rs": py * 8 + zl * 2 + core}

    load_i = pltpu.make_async_copy(i_hbm, i_v, in_sems.at[0])
    load_b = pltpu.make_async_copy(b_hbm, blk_v, in_sems.at[1])
    load_b.start()
    load_i.start()
    barrier = pltpu.get_barrier_semaphore()

    def greet(peer):
        def one(k, _):
            pl.semaphore_signal(barrier, inc=1, device_id=peer(k), device_id_type=MESH)
            return 0

        return one

    z_v[...] = jnp.zeros(z_v.shape, BF16)
    b_v[...] = jnp.zeros(b_v.shape, BF16)
    lax.fori_loop(1, 16, greet(column_peer), 0)
    lax.fori_loop(1, 16, greet(plane_peer), 0)

    load_b.wait()
    b_v[:, :, 0:112] = blk_v[...].reshape(9, 4, 112)
    spot = zh * 96 + y * 8 + (zl * 2 + core) * 9
    z_v[pl.ds(spot, 9)] = b_v[...]
    pl.semaphore_wait(barrier, 30)

    def send_block(n, _):
        k = (n + 7) % 15 + 1
        pltpu.make_async_remote_copy(
            src_ref=b_v, dst_ref=z_v.at[pl.ds(spot, 9)], send_sem=zsend, recv_sem=zrecv,
            device_id=column_peer(k), device_id_type=MESH,
        ).start()
        return 0

    lax.fori_loop(0, 15, send_block, 0)
    order = one_hot((128, 128), lambda n: jnp.where(n < 112, ((n // 2) % 4) * 28 + (n // 8) * 2 + n % 2, -1))
    perm_v[...] = one_hot(
        perm_v.shape, lambda n: ((n // 8) % 8) * 112 + ((n // 2) % 4) * 28 + (n // 64) * 2 + n % 2
    )
    pltpu.make_async_copy(z_v.at[pl.ds(0, 135)], z_v.at[pl.ds(0, 135)], zrecv).wait()
    mine = x * 4 + y

    def spread(q):
        def one(n, _):
            k = (n + 9) % 15 + 1
            pltpu.make_async_remote_copy(
                src_ref=at_v.at[q], dst_ref=g_v.at[q, mine], send_sem=gsend.at[q], recv_sem=grecv.at[q],
                device_id=plane_peer(k), device_id_type=MESH,
            ).start()
            return 0

        lax.fori_loop(0, 15, one, 0)

    strips = [z_v[pl.ds(h * 96, 96)].reshape(384, 128) for h in range(2)]

    def turned(h, rows):
        return lax.dot_general(rows, strips[h], (((1,), (1,)), ((), ())), preferred_element_type=F32).astype(BF16)

    for h in range(2):
        at_v[0, h] = turned(h, order[0:16])[0:8]
    spread(0)
    for h in range(2):
        rest = turned(h, order)
        for q in range(1, CHUNKS):
            at_v[q, h] = rest[q * 8 : (q + 1) * 8]
    for q in range(1, DIRECT):
        spread(q)

    def line(n, _):
        pltpu.make_async_remote_copy(
            src_ref=at_v.at[pl.ds(DIRECT, CHUNKS - DIRECT)], dst_ref=g_v.at[pl.ds(DIRECT, CHUNKS - DIRECT), mine], send_sem=ysend,
            recv_sem=yrecv, device_id={"rs": ((y + 1 + (n + 1) % 3) % 4) * 8 + zl * 2 + core}, device_id_type=MESH,
        ).start()
        return 0

    lax.fori_loop(0, 3, line, 0)
    g_v[:, mine] = at_v[...]
    load_i.wait()

    def across(q, _):
        for n in (2, 1, 3):
            lane = g_v.at[q, pl.ds(x * 4, 4)]
            pltpu.make_async_remote_copy(
                src_ref=lane, dst_ref=lane, send_sem=gsend.at[q], recv_sem=grecv.at[q],
                device_id={"pq": zh * 4 + (x + n) % 4}, device_id_type=MESH,
            ).start()
        return 0

    def arrived(q, blocks, sems):
        pltpu.make_async_copy(g_v.at[q, pl.ds(0, blocks)], g_v.at[q, pl.ds(0, blocks)], sems.at[q]).wait()

    def three_lines(sem):
        every = g_v.at[pl.ds(0, CHUNKS - DIRECT), pl.ds(0, 3)]
        pltpu.make_async_copy(every, every, sem).wait()

    def assemble(q):
        rows = pl.ds(pl.multiple_of(q * 64, 64), 64)
        windows = [
            jnp.concatenate([g_v[q, px * 4 + w, h] for h in range(2) for px in range(4)], axis=0) for w in range(4)
        ]
        for t in range(9):
            parts = [windows[w][:, (t - 2 * w) * 128 : (t - 2 * w + 1) * 128] for w in range(4) if 0 <= t - 2 * w < 3]
            pt_v[rows, t * 128 : (t + 1) * 128] = sum(parts[1:], parts[0])

    def columns(q, u):
        rows = pl.ds(pl.multiple_of(q * 64, 64), 64)
        for v in range(3):
            g = u * 3 + v
            acc = lax.dot_general(
                pt_v[rows, :], i_v[pl.ds(pl.multiple_of(g * 256, 256), 256), :], (((1,), (1,)), ((), ())),
                preferred_element_type=F32,
            )
            for h in range(2):
                tile = swapped(acc[:, h * 128 : (h + 1) * 128]).astype(BF16)
                s_v[q, :, 2 * g + h] = tile.reshape(32, 2, 128)

    def exchange(q, start, size):
        part = pl.ds(start, size)

        def issue(k, _):
            d = (rs + k) % 32
            pltpu.make_async_remote_copy(
                src_ref=s_v.at[q, d, part], dst_ref=r_v.at[q, rs, part], send_sem=send_sems.at[q],
                recv_sem=recv_sems.at[q], device_id={"rs": d}, device_id_type=MESH,
            ).start()
            return 0

        lax.fori_loop(1, 32, issue, 0)

    arrived(0, 15, grecv)
    assemble(0)
    for u in range(3):
        columns(0, u)
        exchange(0, u * 6, 6)
    r_v[0, rs] = s_v[0, rs]

    def first(blocks, q, _):
        arrived(q, blocks, grecv)
        assemble(q)

        def some(u, _):
            columns(q, u)
            return 0

        lax.fori_loop(0, 3, some, 0)
        exchange(q, 0, 18)
        r_v[q, rs] = s_v[q, rs]
        return 0

    lax.fori_loop(1, DIRECT, functools.partial(first, 15), 0)
    three_lines(yrecv)
    lax.fori_loop(DIRECT, CHUNKS, across, 0)
    lax.fori_loop(DIRECT, CHUNKS, functools.partial(first, 12), 0)

    def natural(g, _):
        rows = pl.ds(pl.multiple_of(g * 128, 128), 128)
        acc = lax.dot_general(pt_v[:, rows], perm_v[...], (((0,), (0,)), ((), ())), preferred_element_type=F32)
        c_v[rows, :] = acc.astype(BF16)
        return 0

    lax.fori_loop(0, 9, natural, 0)

    def second(q, _):
        pltpu.make_async_copy(r_v.at[q, pl.ds(0, 31)], r_v.at[q, pl.ds(0, 31)], recv_sems.at[q]).wait()
        tiles = r_v[q].reshape(NBASIS, 128)
        acc = lax.dot_general(tiles, c_v[...], (((0,), (0,)), ((), ())), preferred_element_type=F32)
        o_ref[q] = acc.astype(BF16)
        return 0

    lax.fori_loop(0, CHUNKS, second, 0)

    def drain(q, _):
        pltpu.make_async_copy(s_v.at[q, pl.ds(0, 31)], s_v.at[q, pl.ds(0, 31)], send_sems.at[q]).wait()
        return 0

    lax.fori_loop(0, CHUNKS, drain, 0)
    for q in range(CHUNKS):
        arrived(q, 15 if q < DIRECT else 12, gsend)
    three_lines(ysend)
    pltpu.make_async_copy(z_v.at[pl.ds(0, 135)], z_v.at[pl.ds(0, 135)], zsend).wait()


NBASIS = 1152
NORB = 896


def transform(flat, block):
    far = pl.BlockSpec(memory_space=pltpu.HBM)
    dma = pltpu.SemaphoreType.DMA
    return pl.pallas_call(
        kernel,
        out_shape=jax.ShapeDtypeStruct((CHUNKS, 128, NORB), BF16),
        in_specs=[far, far],
        out_specs=pl.BlockSpec(memory_space=pltpu.VMEM),
        scratch_shapes=[
            pltpu.VMEM((2304, NBASIS), BF16),
            pltpu.VMEM((36, 112), BF16),
            pltpu.VMEM((9, 4, 128), BF16),
            pltpu.VMEM((192, 4, 128), BF16),
            pltpu.VMEM((CHUNKS, 2, 8, 384), BF16),
            pltpu.VMEM((CHUNKS, 16, 2, 8, 384), BF16),
            pltpu.VMEM((NORB, NBASIS), BF16),
            pltpu.VMEM((NORB, NORB), BF16),
            pltpu.VMEM((NBASIS, NORB), BF16),
            pltpu.VMEM((CHUNKS, 32, 18, 2, 128), BF16),
            pltpu.VMEM((CHUNKS, 32, 18, 2, 128), BF16),
            dma((2,)),
            dma,
            dma,
            dma,
            dma,
            dma((CHUNKS,)),
            dma((CHUNKS,)),
            dma((CHUNKS,)),
            dma((CHUNKS,)),
        ],
        compiler_params=pltpu.CompilerParams(collective_id=0, has_side_effects=True, vmem_limit_bytes=48 * 2**20),
        name="half",
    )(flat, block)


def on_device(integrals, coeff):
    flat = integrals.transpose(1, 0, 2).reshape(2304, NBASIS)
    return transform(flat, pltpu.with_memory_space_constraint(coeff, pltpu.HBM)).reshape(28, 64, NORB).transpose(1, 0, 2)


def solution(mesh):
    placed = (P("pq", "rs", None), P("rs", "pq"))
    return jax.shard_map(on_device, mesh=mesh, in_specs=placed, out_specs=P("pq", "rs", None), check_vma=False)
```

```python
import functools

import jax
import jax.numpy as jnp
from jax import lax
from jax.experimental import pallas as pl
from jax.experimental.pallas import tpu as pltpu
from jax.sharding import PartitionSpec as P

MESH = pl.DeviceIdType.MESH
BF16 = jnp.bfloat16
F32 = jnp.float32
CHUNKS = 14
DIRECT = 3


def one_hot(shape, column_of_row):
    rows = lax.broadcasted_iota(jnp.int32, shape, 0)
    columns = lax.broadcasted_iota(jnp.int32, shape, 1)
    return jnp.where(column_of_row(rows) == columns, 1.0, 0.0).astype(BF16)


def swapped(tile):
    rows = lax.broadcasted_iota(jnp.int32, tile.shape, 0) % 2
    lanes = lax.broadcasted_iota(jnp.int32, tile.shape, 1) // 64
    turned = pltpu.roll(tile, 64, 1)
    above = pltpu.roll(turned, tile.shape[0] - 1, 0)
    below = pltpu.roll(turned, 1, 0)
    return jnp.where(rows == lanes, tile, jnp.where(rows == 0, above, below))


def kernel(
    i_hbm, b_hbm, o_ref,
    i_v, blk_v, b_v, z_v, at_v, g_v, pt_v, perm_v, c_v, s_v, r_v,
    in_sems, zsend, zrecv, ysend, yrecv, gsend, grecv, send_sems, recv_sems,
):
    pq, rs = lax.axis_index("pq"), lax.axis_index("rs")
    zh, x = pq // 4, pq % 4
    y, zl, core = rs // 8, (rs // 2) % 4, rs % 2
    z = zh * 4 + zl

    def column_peer(k):
        pz, pc = (z + k // 2) % 8, (core + k) % 2
        return {"pq": (pz // 4) * 4 + x, "rs": y * 8 + (pz % 4) * 2 + pc}

    def plane_peer(k):
        py, px = (y + k // 4) % 4, (x + k) % 4
        return {"pq": zh * 4 + px, "rs": py * 8 + zl * 2 + core}

    load_i = pltpu.make_async_copy(i_hbm, i_v, in_sems.at[0])
    load_b = pltpu.make_async_copy(b_hbm, blk_v, in_sems.at[1])
    load_b.start()
    load_i.start()
    barrier = pltpu.get_barrier_semaphore()

    def greet(peer):
        def one(k, _):
            pl.semaphore_signal(barrier, inc=1, device_id=peer(k), device_id_type=MESH)
            return 0

        return one

    z_v[...] = jnp.zeros(z_v.shape, BF16)
    b_v[...] = jnp.zeros(b_v.shape, BF16)
    lax.fori_loop(1, 16, greet(column_peer), 0, unroll=True)
    lax.fori_loop(1, 16, greet(plane_peer), 0, unroll=True)

    load_b.wait()
    b_v[:, :, 0:112] = blk_v[...].reshape(9, 4, 112)
    spot = zh * 96 + y * 8 + (zl * 2 + core) * 9
    z_v[pl.ds(spot, 9)] = b_v[...]
    pl.semaphore_wait(barrier, 30)

    def send_block(n, _):
        k = (n + 7) % 15 + 1
        pltpu.make_async_remote_copy(
            src_ref=b_v, dst_ref=z_v.at[pl.ds(spot, 9)], send_sem=zsend, recv_sem=zrecv,
            device_id=column_peer(k), device_id_type=MESH,
        ).start()
        return 0

    lax.fori_loop(0, 15, send_block, 0, unroll=True)
    order = one_hot((128, 128), lambda n: jnp.where(n < 112, ((n // 2) % 4) * 28 + (n // 8) * 2 + n % 2, -1))
    perm_v[...] = one_hot(
        perm_v.shape, lambda n: ((n // 8) % 8) * 112 + ((n // 2) % 4) * 28 + (n // 64) * 2 + n % 2
    )
    pltpu.make_async_copy(z_v.at[pl.ds(0, 135)], z_v.at[pl.ds(0, 135)], zrecv).wait()
    mine = x * 4 + y

    def spread(q):
        def one(n, _):
            k = (n + 9) % 15 + 1
            pltpu.make_async_remote_copy(
                src_ref=at_v.at[q], dst_ref=g_v.at[q, mine], send_sem=gsend.at[q], recv_sem=grecv.at[q],
                device_id=plane_peer(k), device_id_type=MESH,
            ).start()
            return 0

        lax.fori_loop(0, 15, one, 0, unroll=True)

    strips = [z_v[pl.ds(h * 96, 96)].reshape(384, 128) for h in range(2)]

    def turned(h, rows):
        return lax.dot_general(rows, strips[h], (((1,), (1,)), ((), ())), preferred_element_type=F32).astype(BF16)

    for h in range(2):
        at_v[0, h] = turned(h, order[0:16])[0:8]
    spread(0)
    for h in range(2):
        rest = turned(h, order)
        for q in range(1, CHUNKS):
            at_v[q, h] = rest[q * 8 : (q + 1) * 8]
    for q in range(1, DIRECT):
        spread(q)

    def line(n, _):
        pltpu.make_async_remote_copy(
            src_ref=at_v.at[pl.ds(DIRECT, CHUNKS - DIRECT)], dst_ref=g_v.at[pl.ds(DIRECT, CHUNKS - DIRECT), mine], send_sem=ysend,
            recv_sem=yrecv, device_id={"rs": ((y + 1 + (n + 1) % 3) % 4) * 8 + zl * 2 + core}, device_id_type=MESH,
        ).start()
        return 0

    lax.fori_loop(0, 3, line, 0)
    g_v[:, mine] = at_v[...]
    load_i.wait()

    def across(q, _):
        for n in (2, 1, 3):
            lane = g_v.at[q, pl.ds(x * 4, 4)]
            pltpu.make_async_remote_copy(
                src_ref=lane, dst_ref=lane, send_sem=gsend.at[q], recv_sem=grecv.at[q],
                device_id={"pq": zh * 4 + (x + n) % 4}, device_id_type=MESH,
            ).start()
        return 0

    def arrived(q, blocks, sems):
        pltpu.make_async_copy(g_v.at[q, pl.ds(0, blocks)], g_v.at[q, pl.ds(0, blocks)], sems.at[q]).wait()

    def three_lines(sem):
        every = g_v.at[pl.ds(0, CHUNKS - DIRECT), pl.ds(0, 3)]
        pltpu.make_async_copy(every, every, sem).wait()

    def assemble(q):
        rows = pl.ds(pl.multiple_of(q * 64, 64), 64)
        windows = [
            jnp.concatenate([g_v[q, px * 4 + w, h] for h in range(2) for px in range(4)], axis=0) for w in range(4)
        ]
        for t in range(9):
            parts = [windows[w][:, (t - 2 * w) * 128 : (t - 2 * w + 1) * 128] for w in range(4) if 0 <= t - 2 * w < 3]
            pt_v[rows, t * 128 : (t + 1) * 128] = sum(parts[1:], parts[0])

    def columns(q, u):
        rows = pl.ds(pl.multiple_of(q * 64, 64), 64)
        for v in range(3):
            g = u * 3 + v
            acc = lax.dot_general(
                pt_v[rows, :], i_v[pl.ds(pl.multiple_of(g * 256, 256), 256), :], (((1,), (1,)), ((), ())),
                preferred_element_type=F32,
            )
            for h in range(2):
                tile = swapped(acc[:, h * 128 : (h + 1) * 128]).astype(BF16)
                s_v[q, :, 2 * g + h] = tile.reshape(32, 2, 128)

    def exchange(q, start, size):
        part = pl.ds(start, size)

        def issue(k, _):
            d = (rs + k + core * (32 - 2 * k)) % 32
            pltpu.make_async_remote_copy(
                src_ref=s_v.at[q, d, part], dst_ref=r_v.at[q, rs, part], send_sem=send_sems.at[q],
                recv_sem=recv_sems.at[q], device_id={"rs": d}, device_id_type=MESH,
            ).start()
            return 0

        lax.fori_loop(1, 32, issue, 0, unroll=size < 18)

    arrived(0, 15, grecv)
    assemble(0)
    for u in range(3):
        columns(0, u)
        exchange(0, u * 6, 6)
    r_v[0, rs] = s_v[0, rs]

    def first(blocks, q, _):
        arrived(q, blocks, grecv)
        assemble(q)

        def some(u, _):
            columns(q, u)
            return 0

        lax.fori_loop(0, 3, some, 0)
        exchange(q, 0, 18)
        r_v[q, rs] = s_v[q, rs]
        return 0

    lax.fori_loop(1, DIRECT, functools.partial(first, 15), 0)
    three_lines(yrecv)
    lax.fori_loop(DIRECT, CHUNKS, across, 0)
    lax.fori_loop(DIRECT, CHUNKS, functools.partial(first, 12), 0)

    def natural(g, _):
        rows = pl.ds(pl.multiple_of(g * 128, 128), 128)
        acc = lax.dot_general(pt_v[:, rows], perm_v[...], (((0,), (0,)), ((), ())), preferred_element_type=F32)
        c_v[rows, :] = acc.astype(BF16)
        return 0

    lax.fori_loop(0, 9, natural, 0)

    def second(q, _):
        pltpu.make_async_copy(r_v.at[q, pl.ds(0, 31)], r_v.at[q, pl.ds(0, 31)], recv_sems.at[q]).wait()
        tiles = r_v[q].reshape(NBASIS, 128)
        acc = lax.dot_general(tiles, c_v[...], (((0,), (0,)), ((), ())), preferred_element_type=F32)
        o_ref[q] = acc.astype(BF16)
        return 0

    lax.fori_loop(0, CHUNKS, second, 0)

    def drain(q, _):
        pltpu.make_async_copy(s_v.at[q, pl.ds(0, 31)], s_v.at[q, pl.ds(0, 31)], send_sems.at[q]).wait()
        return 0

    lax.fori_loop(0, CHUNKS, drain, 0)
    for q in range(CHUNKS):
        arrived(q, 15 if q < DIRECT else 12, gsend)
    three_lines(ysend)
    pltpu.make_async_copy(z_v.at[pl.ds(0, 135)], z_v.at[pl.ds(0, 135)], zsend).wait()


NBASIS = 1152
NORB = 896


def transform(flat, block):
    far = pl.BlockSpec(memory_space=pltpu.HBM)
    dma = pltpu.SemaphoreType.DMA
    return pl.pallas_call(
        kernel,
        out_shape=jax.ShapeDtypeStruct((CHUNKS, 128, NORB), BF16),
        in_specs=[far, far],
        out_specs=pl.BlockSpec(memory_space=pltpu.VMEM),
        scratch_shapes=[
            pltpu.VMEM((2304, NBASIS), BF16),
            pltpu.VMEM((36, 112), BF16),
            pltpu.VMEM((9, 4, 128), BF16),
            pltpu.VMEM((192, 4, 128), BF16),
            pltpu.VMEM((CHUNKS, 2, 8, 384), BF16),
            pltpu.VMEM((CHUNKS, 16, 2, 8, 384), BF16),
            pltpu.VMEM((NORB, NBASIS), BF16),
            pltpu.VMEM((NORB, NORB), BF16),
            pltpu.VMEM((NBASIS, NORB), BF16),
            pltpu.VMEM((CHUNKS, 32, 18, 2, 128), BF16),
            pltpu.VMEM((CHUNKS, 32, 18, 2, 128), BF16),
            dma((2,)),
            dma,
            dma,
            dma,
            dma,
            dma((CHUNKS,)),
            dma((CHUNKS,)),
            dma((CHUNKS,)),
            dma((CHUNKS,)),
        ],
        compiler_params=pltpu.CompilerParams(collective_id=0, has_side_effects=True, vmem_limit_bytes=48 * 2**20),
        name="half",
    )(flat, block)


def on_device(integrals, coeff):
    flat = integrals.transpose(1, 0, 2).reshape(2304, NBASIS)
    return transform(flat, pltpu.with_memory_space_constraint(coeff, pltpu.HBM)).reshape(28, 64, NORB).transpose(1, 0, 2)


def solution(mesh):
    placed = (P("pq", "rs", None), P("rs", "pq"))
    return jax.shard_map(on_device, mesh=mesh, in_specs=placed, out_specs=P("pq", "rs", None), check_vma=False)
```

```python
import functools

import jax
import jax.numpy as jnp
from jax import lax
from jax.experimental import pallas as pl
from jax.experimental.pallas import tpu as pltpu
from jax.sharding import PartitionSpec as P

MESH = pl.DeviceIdType.MESH
BF16 = jnp.bfloat16
F32 = jnp.float32
CHUNKS = 14
DIRECT = 3


def one_hot(shape, column_of_row):
    rows = lax.broadcasted_iota(jnp.int32, shape, 0)
    columns = lax.broadcasted_iota(jnp.int32, shape, 1)
    return jnp.where(column_of_row(rows) == columns, 1.0, 0.0).astype(BF16)


def swapped(tile):
    rows = lax.broadcasted_iota(jnp.int32, tile.shape, 0) % 2
    lanes = lax.broadcasted_iota(jnp.int32, tile.shape, 1) // 64
    turned = pltpu.roll(tile, 64, 1)
    above = pltpu.roll(turned, tile.shape[0] - 1, 0)
    below = pltpu.roll(turned, 1, 0)
    return jnp.where(rows == lanes, tile, jnp.where(rows == 0, above, below))


def kernel(
    i_hbm, b_hbm, o_ref,
    i_v, blk_v, b_v, z_v, at_v, g_v, pt_v, perm_v, c_v, s_v, r_v,
    in_sems, zsend, zrecv, ysend, yrecv, gsend, grecv, send_sems, recv_sems,
):
    pq, rs = lax.axis_index("pq"), lax.axis_index("rs")
    zh, x = pq // 4, pq % 4
    y, zl, core = rs // 8, (rs // 2) % 4, rs % 2
    z = zh * 4 + zl

    def column_peer(k):
        pz, pc = (z + k // 2) % 8, (core + k) % 2
        return {"pq": (pz // 4) * 4 + x, "rs": y * 8 + (pz % 4) * 2 + pc}

    def plane_peer(k):
        py, px = (y + k // 4) % 4, (x + k) % 4
        return {"pq": zh * 4 + px, "rs": py * 8 + zl * 2 + core}

    load_i = pltpu.make_async_copy(i_hbm, i_v, in_sems.at[0])
    load_b = pltpu.make_async_copy(b_hbm, blk_v, in_sems.at[1])
    load_b.start()
    load_i.start()
    barrier = pltpu.get_barrier_semaphore()

    def greet(peer):
        def one(k, _):
            pl.semaphore_signal(barrier, inc=1, device_id=peer(k), device_id_type=MESH)
            return 0

        return one

    z_v[...] = jnp.zeros(z_v.shape, BF16)
    b_v[...] = jnp.zeros(b_v.shape, BF16)
    lax.fori_loop(1, 16, greet(column_peer), 0, unroll=True)
    lax.fori_loop(1, 16, greet(plane_peer), 0, unroll=True)

    load_b.wait()
    b_v[:, :, 0:112] = blk_v[...].reshape(9, 4, 112)
    spot = zh * 96 + y * 8 + (zl * 2 + core) * 9
    z_v[pl.ds(spot, 9)] = b_v[...]
    pl.semaphore_wait(barrier, 30)

    def send_block(n, _):
        k = (n + 7) % 15 + 1
        pltpu.make_async_remote_copy(
            src_ref=b_v, dst_ref=z_v.at[pl.ds(spot, 9)], send_sem=zsend, recv_sem=zrecv,
            device_id=column_peer(k), device_id_type=MESH,
        ).start()
        return 0

    lax.fori_loop(0, 15, send_block, 0, unroll=True)
    order = one_hot((128, 128), lambda n: jnp.where(n < 112, ((n // 2) % 4) * 28 + (n // 8) * 2 + n % 2, -1))
    perm_v[...] = one_hot(
        perm_v.shape, lambda n: ((n // 8) % 8) * 112 + ((n // 2) % 4) * 28 + (n // 64) * 2 + n % 2
    )
    pltpu.make_async_copy(z_v.at[pl.ds(0, 135)], z_v.at[pl.ds(0, 135)], zrecv).wait()
    mine = x * 4 + y

    def spread(q):
        def one(n, _):
            k = (n + 9) % 15 + 1
            pltpu.make_async_remote_copy(
                src_ref=at_v.at[q], dst_ref=g_v.at[q, mine], send_sem=gsend.at[q], recv_sem=grecv.at[q],
                device_id=plane_peer(k), device_id_type=MESH,
            ).start()
            return 0

        lax.fori_loop(0, 15, one, 0, unroll=True)

    strips = [z_v[pl.ds(h * 96, 96)].reshape(384, 128) for h in range(2)]

    def turned(h, rows):
        return lax.dot_general(rows, strips[h], (((1,), (1,)), ((), ())), preferred_element_type=F32).astype(BF16)

    for h in range(2):
        at_v[0, h] = turned(h, order[0:16])[0:8]
    spread(0)
    for h in range(2):
        rest = turned(h, order)
        for q in range(1, CHUNKS):
            at_v[q, h] = rest[q * 8 : (q + 1) * 8]
    for q in range(1, DIRECT):
        spread(q)

    def line(n, _):
        pltpu.make_async_remote_copy(
            src_ref=at_v.at[pl.ds(DIRECT, CHUNKS - DIRECT)], dst_ref=g_v.at[pl.ds(DIRECT, CHUNKS - DIRECT), mine], send_sem=ysend,
            recv_sem=yrecv, device_id={"rs": ((y + 1 + (n + 1) % 3) % 4) * 8 + zl * 2 + core}, device_id_type=MESH,
        ).start()
        return 0

    lax.fori_loop(0, 3, line, 0)
    g_v[:, mine] = at_v[...]
    load_i.wait()

    def across(q, _):
        for n in (2, 1, 3):
            lane = g_v.at[q, pl.ds(x * 4, 4)]
            pltpu.make_async_remote_copy(
                src_ref=lane, dst_ref=lane, send_sem=gsend.at[q], recv_sem=grecv.at[q],
                device_id={"pq": zh * 4 + (x + n) % 4}, device_id_type=MESH,
            ).start()
        return 0

    def arrived(q, blocks, sems):
        pltpu.make_async_copy(g_v.at[q, pl.ds(0, blocks)], g_v.at[q, pl.ds(0, blocks)], sems.at[q]).wait()

    def three_lines(sem):
        every = g_v.at[pl.ds(0, CHUNKS - DIRECT), pl.ds(0, 3)]
        pltpu.make_async_copy(every, every, sem).wait()

    def assemble(q):
        rows = pl.ds(pl.multiple_of(q * 64, 64), 64)
        windows = [
            jnp.concatenate([g_v[q, px * 4 + w, h] for h in range(2) for px in range(4)], axis=0) for w in range(4)
        ]
        for t in range(9):
            parts = [windows[w][:, (t - 2 * w) * 128 : (t - 2 * w + 1) * 128] for w in range(4) if 0 <= t - 2 * w < 3]
            pt_v[rows, t * 128 : (t + 1) * 128] = sum(parts[1:], parts[0])

    def columns(q, u):
        rows = pl.ds(pl.multiple_of(q * 64, 64), 64)
        for v in range(3):
            g = u * 3 + v
            acc = lax.dot_general(
                pt_v[rows, :], i_v[pl.ds(pl.multiple_of(g * 256, 256), 256), :], (((1,), (1,)), ((), ())),
                preferred_element_type=F32,
            )
            for h in range(2):
                tile = swapped(acc[:, h * 128 : (h + 1) * 128]).astype(BF16)
                s_v[q, :, 2 * g + h] = tile.reshape(32, 2, 128)

    def exchange(q, start, size):
        part = pl.ds(start, size)

        def issue(k, _):
            d = (rs + k + core * (32 - 2 * k)) % 32
            pltpu.make_async_remote_copy(
                src_ref=s_v.at[q, d, part], dst_ref=r_v.at[q, rs, part], send_sem=send_sems.at[q],
                recv_sem=recv_sems.at[q], device_id={"rs": d}, device_id_type=MESH,
            ).start()
            return 0

        lax.fori_loop(1, 32, issue, 0, unroll=size < 18)

    arrived(0, 15, grecv)
    assemble(0)
    for u in range(3):
        columns(0, u)
        exchange(0, u * 6, 6)
    r_v[0, rs] = s_v[0, rs]

    def first(blocks, q, _):
        arrived(q, blocks, grecv)
        assemble(q)

        def some(u, _):
            columns(q, u)
            return 0

        lax.fori_loop(0, 3, some, 0)
        exchange(q, 0, 18)
        r_v[q, rs] = s_v[q, rs]
        return 0

    lax.fori_loop(1, DIRECT, functools.partial(first, 15), 0)
    three_lines(yrecv)
    lax.fori_loop(DIRECT, CHUNKS, across, 0)
    lax.fori_loop(DIRECT, CHUNKS, functools.partial(first, 12), 0)

    def natural(g, _):
        rows = pl.ds(pl.multiple_of(g * 128, 128), 128)
        acc = lax.dot_general(pt_v[:, rows], perm_v[...], (((0,), (0,)), ((), ())), preferred_element_type=F32)
        c_v[rows, :] = acc.astype(BF16)
        return 0

    lax.fori_loop(0, 9, natural, 0)
    for q in range(CHUNKS):
        arrived(q, 15 if q < DIRECT else 12, gsend)
    three_lines(ysend)
    pltpu.make_async_copy(z_v.at[pl.ds(0, 135)], z_v.at[pl.ds(0, 135)], zsend).wait()

    def second(q, _):
        pltpu.make_async_copy(r_v.at[q, pl.ds(0, 31)], r_v.at[q, pl.ds(0, 31)], recv_sems.at[q]).wait()
        tiles = r_v[q].reshape(NBASIS, 128)
        acc = lax.dot_general(tiles, c_v[...], (((0,), (0,)), ((), ())), preferred_element_type=F32)
        o_ref[q] = acc.astype(BF16)
        return 0

    def drain(q, _):
        pltpu.make_async_copy(s_v.at[q, pl.ds(0, 31)], s_v.at[q, pl.ds(0, 31)], send_sems.at[q]).wait()
        return 0

    lax.fori_loop(0, CHUNKS - 1, second, 0)
    lax.fori_loop(0, CHUNKS - 1, drain, 0)
    second(CHUNKS - 1, 0)
    drain(CHUNKS - 1, 0)


NBASIS = 1152
NORB = 896


def transform(flat, block):
    far = pl.BlockSpec(memory_space=pltpu.HBM)
    dma = pltpu.SemaphoreType.DMA
    return pl.pallas_call(
        kernel,
        out_shape=jax.ShapeDtypeStruct((CHUNKS, 128, NORB), BF16),
        in_specs=[far, far],
        out_specs=pl.BlockSpec(memory_space=pltpu.VMEM),
        scratch_shapes=[
            pltpu.VMEM((2304, NBASIS), BF16),
            pltpu.VMEM((36, 112), BF16),
            pltpu.VMEM((9, 4, 128), BF16),
            pltpu.VMEM((192, 4, 128), BF16),
            pltpu.VMEM((CHUNKS, 2, 8, 384), BF16),
            pltpu.VMEM((CHUNKS, 16, 2, 8, 384), BF16),
            pltpu.VMEM((NORB, NBASIS), BF16),
            pltpu.VMEM((NORB, NORB), BF16),
            pltpu.VMEM((NBASIS, NORB), BF16),
            pltpu.VMEM((CHUNKS, 32, 18, 2, 128), BF16),
            pltpu.VMEM((CHUNKS, 32, 18, 2, 128), BF16),
            dma((2,)),
            dma,
            dma,
            dma,
            dma,
            dma((CHUNKS,)),
            dma((CHUNKS,)),
            dma((CHUNKS,)),
            dma((CHUNKS,)),
        ],
        compiler_params=pltpu.CompilerParams(collective_id=0, has_side_effects=True, vmem_limit_bytes=48 * 2**20),
        name="half",
    )(flat, block)


def on_device(integrals, coeff):
    flat = integrals.transpose(1, 0, 2).reshape(2304, NBASIS)
    return transform(flat, pltpu.with_memory_space_constraint(coeff, pltpu.HBM)).reshape(28, 64, NORB).transpose(1, 0, 2)


def solution(mesh):
    placed = (P("pq", "rs", None), P("rs", "pq"))
    return jax.shard_map(on_device, mesh=mesh, in_specs=placed, out_specs=P("pq", "rs", None), check_vma=False)
```

```python
import functools

import jax
import jax.numpy as jnp
from jax import lax
from jax.experimental import pallas as pl
from jax.experimental.pallas import tpu as pltpu
from jax.sharding import PartitionSpec as P

MESH = pl.DeviceIdType.MESH
BF16 = jnp.bfloat16
F32 = jnp.float32
CHUNKS = 14
DIRECT = 3


def one_hot(shape, column_of_row):
    rows = lax.broadcasted_iota(jnp.int32, shape, 0)
    columns = lax.broadcasted_iota(jnp.int32, shape, 1)
    return jnp.where(column_of_row(rows) == columns, 1.0, 0.0).astype(BF16)


def swapped(tile):
    rows = lax.broadcasted_iota(jnp.int32, tile.shape, 0) % 2
    lanes = lax.broadcasted_iota(jnp.int32, tile.shape, 1) // 64
    turned = pltpu.roll(tile, 64, 1)
    above = pltpu.roll(turned, tile.shape[0] - 1, 0)
    below = pltpu.roll(turned, 1, 0)
    return jnp.where(rows == lanes, tile, jnp.where(rows == 0, above, below))


def kernel(
    i_hbm, b_hbm, o_ref,
    i_v, blk_v, b_v, z_v, at_v, g_v, pt_v, perm_v, c_v, s_v, r_v,
    in_sems, zsend, zrecv, ysend, yrecv, gsend, grecv, send_sems, recv_sems,
):
    pq, rs = lax.axis_index("pq"), lax.axis_index("rs")
    zh, x = pq // 4, pq % 4
    y, zl, core = rs // 8, (rs // 2) % 4, rs % 2
    z = zh * 4 + zl

    def column_peer(k):
        pz, pc = (z + k // 2) % 8, (core + k) % 2
        return {"pq": (pz // 4) * 4 + x, "rs": y * 8 + (pz % 4) * 2 + pc}

    def plane_peer(k):
        py, px = (y + k // 4) % 4, (x + k) % 4
        return {"pq": zh * 4 + px, "rs": py * 8 + zl * 2 + core}

    load_i = pltpu.make_async_copy(i_hbm, i_v, in_sems.at[0])
    load_b = pltpu.make_async_copy(b_hbm, blk_v, in_sems.at[1])
    load_b.start()
    load_i.start()
    barrier = pltpu.get_barrier_semaphore()

    def greet(peer):
        def one(k, _):
            pl.semaphore_signal(barrier, inc=1, device_id=peer(k), device_id_type=MESH)
            return 0

        return one

    z_v[...] = jnp.zeros(z_v.shape, BF16)
    b_v[...] = jnp.zeros(b_v.shape, BF16)
    lax.fori_loop(1, 16, greet(column_peer), 0, unroll=True)
    lax.fori_loop(1, 16, greet(plane_peer), 0, unroll=True)

    load_b.wait()
    b_v[:, :, 0:112] = blk_v[...].reshape(9, 4, 112)
    spot = zh * 96 + y * 8 + (zl * 2 + core) * 9
    z_v[pl.ds(spot, 9)] = b_v[...]
    pl.semaphore_wait(barrier, 30)

    def send_block(n, _):
        k = (n + 7) % 15 + 1
        pltpu.make_async_remote_copy(
            src_ref=b_v, dst_ref=z_v.at[pl.ds(spot, 9)], send_sem=zsend, recv_sem=zrecv,
            device_id=column_peer(k), device_id_type=MESH,
        ).start()
        return 0

    lax.fori_loop(0, 15, send_block, 0, unroll=True)
    order = one_hot((128, 128), lambda n: jnp.where(n < 112, ((n // 2) % 4) * 28 + (n // 8) * 2 + n % 2, -1))
    perm_v[...] = one_hot(
        perm_v.shape, lambda n: ((n // 8) % 8) * 112 + ((n // 2) % 4) * 28 + (n // 64) * 2 + n % 2
    )
    pltpu.make_async_copy(z_v.at[pl.ds(0, 135)], z_v.at[pl.ds(0, 135)], zrecv).wait()
    mine = x * 4 + y

    def spread(q):
        def one(n, _):
            k = (n + 9) % 15 + 1
            pltpu.make_async_remote_copy(
                src_ref=at_v.at[q], dst_ref=g_v.at[q, mine], send_sem=gsend.at[q], recv_sem=grecv.at[q],
                device_id=plane_peer(k), device_id_type=MESH,
            ).start()
            return 0

        lax.fori_loop(0, 15, one, 0, unroll=True)

    strips = [z_v[pl.ds(h * 96, 96)].reshape(384, 128) for h in range(2)]

    def turned(h, rows):
        return lax.dot_general(rows, strips[h], (((1,), (1,)), ((), ())), preferred_element_type=F32).astype(BF16)

    for h in range(2):
        at_v[0, h] = turned(h, order[0:16])[0:8]
    spread(0)
    for h in range(2):
        rest = turned(h, order)
        for q in range(1, CHUNKS):
            at_v[q, h] = rest[q * 8 : (q + 1) * 8]
    for q in range(1, DIRECT):
        spread(q)

    def line(n, _):
        pltpu.make_async_remote_copy(
            src_ref=at_v.at[pl.ds(DIRECT, CHUNKS - DIRECT)], dst_ref=g_v.at[pl.ds(DIRECT, CHUNKS - DIRECT), mine], send_sem=ysend,
            recv_sem=yrecv, device_id={"rs": ((y + 1 + (n + 1) % 3) % 4) * 8 + zl * 2 + core}, device_id_type=MESH,
        ).start()
        return 0

    lax.fori_loop(0, 3, line, 0)
    g_v[:, mine] = at_v[...]
    load_i.wait()

    def across(q, _):
        for n in (2, 1, 3):
            lane = g_v.at[q, pl.ds(x * 4, 4)]
            pltpu.make_async_remote_copy(
                src_ref=lane, dst_ref=lane, send_sem=gsend.at[q], recv_sem=grecv.at[q],
                device_id={"pq": zh * 4 + (x + n) % 4}, device_id_type=MESH,
            ).start()
        return 0

    def arrived(q, blocks, sems):
        pltpu.make_async_copy(g_v.at[q, pl.ds(0, blocks)], g_v.at[q, pl.ds(0, blocks)], sems.at[q]).wait()

    def three_lines(sem):
        every = g_v.at[pl.ds(0, CHUNKS - DIRECT), pl.ds(0, 3)]
        pltpu.make_async_copy(every, every, sem).wait()

    def assemble(q):
        rows = pl.ds(pl.multiple_of(q * 64, 64), 64)
        windows = [
            jnp.concatenate([g_v[q, px * 4 + w, h] for h in range(2) for px in range(4)], axis=0) for w in range(4)
        ]
        for t in range(9):
            parts = [windows[w][:, (t - 2 * w) * 128 : (t - 2 * w + 1) * 128] for w in range(4) if 0 <= t - 2 * w < 3]
            pt_v[rows, t * 128 : (t + 1) * 128] = sum(parts[1:], parts[0])

    def columns(q, first_group, groups):
        rows = pl.ds(pl.multiple_of(q * 64, 64), 64)
        for v in range(groups):
            g = first_group + v
            acc = lax.dot_general(
                pt_v[rows, :], i_v[pl.ds(pl.multiple_of(g * 256, 256), 256), :], (((1,), (1,)), ((), ())),
                preferred_element_type=F32,
            )
            for h in range(2):
                tile = swapped(acc[:, h * 128 : (h + 1) * 128]).astype(BF16)
                s_v[q, :, 2 * g + h] = tile.reshape(32, 2, 128)

    def exchange(q, start, size):
        part = pl.ds(start, size)

        def issue(k, _):
            d = (rs + k + core * (32 - 2 * k)) % 32
            pltpu.make_async_remote_copy(
                src_ref=s_v.at[q, d, part], dst_ref=r_v.at[q, rs, part], send_sem=send_sems.at[q],
                recv_sem=recv_sems.at[q], device_id={"rs": d}, device_id_type=MESH,
            ).start()
            return 0

        lax.fori_loop(1, 32, issue, 0, unroll=size < 18)

    arrived(0, 15, grecv)
    assemble(0)
    for start, size in ((0, 2), (2, 3), (5, 4)):
        columns(0, start, size)
        exchange(0, start * 2, size * 2)
    r_v[0, rs] = s_v[0, rs]

    def first(blocks, q, _):
        arrived(q, blocks, grecv)
        assemble(q)

        def some(u, _):
            columns(q, u * 3, 3)
            return 0

        lax.fori_loop(0, 3, some, 0)
        exchange(q, 0, 18)
        r_v[q, rs] = s_v[q, rs]
        return 0

    lax.fori_loop(1, DIRECT, functools.partial(first, 15), 0)
    three_lines(yrecv)
    lax.fori_loop(DIRECT, CHUNKS, across, 0)
    lax.fori_loop(DIRECT, CHUNKS, functools.partial(first, 12), 0)

    def natural(g, _):
        rows = pl.ds(pl.multiple_of(g * 128, 128), 128)
        acc = lax.dot_general(pt_v[:, rows], perm_v[...], (((0,), (0,)), ((), ())), preferred_element_type=F32)
        c_v[rows, :] = acc.astype(BF16)
        return 0

    lax.fori_loop(0, 9, natural, 0)
    for q in range(CHUNKS):
        arrived(q, 15 if q < DIRECT else 12, gsend)
    three_lines(ysend)
    pltpu.make_async_copy(z_v.at[pl.ds(0, 135)], z_v.at[pl.ds(0, 135)], zsend).wait()

    def second(q, _):
        pltpu.make_async_copy(r_v.at[q, pl.ds(0, 31)], r_v.at[q, pl.ds(0, 31)], recv_sems.at[q]).wait()
        tiles = r_v[q].reshape(NBASIS, 128)
        acc = lax.dot_general(tiles, c_v[...], (((0,), (0,)), ((), ())), preferred_element_type=F32)
        o_ref[q] = acc.astype(BF16)
        return 0

    def drain(q, _):
        pltpu.make_async_copy(s_v.at[q, pl.ds(0, 31)], s_v.at[q, pl.ds(0, 31)], send_sems.at[q]).wait()
        return 0

    lax.fori_loop(0, CHUNKS - 1, second, 0)
    lax.fori_loop(0, CHUNKS - 1, drain, 0)
    second(CHUNKS - 1, 0)
    drain(CHUNKS - 1, 0)


NBASIS = 1152
NORB = 896


def transform(flat, block):
    far = pl.BlockSpec(memory_space=pltpu.HBM)
    dma = pltpu.SemaphoreType.DMA
    return pl.pallas_call(
        kernel,
        out_shape=jax.ShapeDtypeStruct((CHUNKS, 128, NORB), BF16),
        in_specs=[far, far],
        out_specs=pl.BlockSpec(memory_space=pltpu.VMEM),
        scratch_shapes=[
            pltpu.VMEM((2304, NBASIS), BF16),
            pltpu.VMEM((36, 112), BF16),
            pltpu.VMEM((9, 4, 128), BF16),
            pltpu.VMEM((192, 4, 128), BF16),
            pltpu.VMEM((CHUNKS, 2, 8, 384), BF16),
            pltpu.VMEM((CHUNKS, 16, 2, 8, 384), BF16),
            pltpu.VMEM((NORB, NBASIS), BF16),
            pltpu.VMEM((NORB, NORB), BF16),
            pltpu.VMEM((NBASIS, NORB), BF16),
            pltpu.VMEM((CHUNKS, 32, 18, 2, 128), BF16),
            pltpu.VMEM((CHUNKS, 32, 18, 2, 128), BF16),
            dma((2,)),
            dma,
            dma,
            dma,
            dma,
            dma((CHUNKS,)),
            dma((CHUNKS,)),
            dma((CHUNKS,)),
            dma((CHUNKS,)),
        ],
        compiler_params=pltpu.CompilerParams(collective_id=0, has_side_effects=True, vmem_limit_bytes=48 * 2**20),
        name="half",
    )(flat, block)


def on_device(integrals, coeff):
    flat = integrals.transpose(1, 0, 2).reshape(2304, NBASIS)
    return transform(flat, pltpu.with_memory_space_constraint(coeff, pltpu.HBM)).reshape(28, 64, NORB).transpose(1, 0, 2)


def solution(mesh):
    placed = (P("pq", "rs", None), P("rs", "pq"))
    return jax.shard_map(on_device, mesh=mesh, in_specs=placed, out_specs=P("pq", "rs", None), check_vma=False)
```
